32 devices in a mesh: dom: 8 (over y, x, core), feat: 4 (over z).
Axes of the slice: x: 2, y: 2, z: 4, core: 2. Of those that a mesh axis runs over, the one named last changes fastest.
Arguments:
- features: bfloat16 [128, 131072], P('feat', 'dom'), may hold values from -6 to 6
- seed_rows: int32 [2048], P('dom'), may hold values from 0 to 16383
- want_rows: int32 [8, 8, 128], P('dom'), may hold values from 0 to 16383
- live_counts: int32 [8, 8], P('dom'), may hold values from 1 to 128, as said below
- hop_one: int32 [15, 2048], P(None, 'dom'), may hold values from 0 to 1023, as said below
- hop_two: int32 [10, 15, 2048], P(None, None, 'dom'), may hold values from 0 to 1023, as said below
- w1_self: bfloat16 [256, 128], replicated, may hold values from -0.5 to 0.5
- w1_neigh: bfloat16 [256, 128], replicated, may hold values from -0.5 to 0.5
- b1: float32 [256], P('feat'), may hold values from -4 to 4
- w2_self: bfloat16 [256, 256], P(None, 'feat'), may hold values from -0.375 to 0.375
- w2_neigh: bfloat16 [256, 256], P(None, 'feat'), may hold values from -0.375 to 0.375
- b2: float32 [256], P('feat'), may hold values from -4 to 4
Outputs:
- embed: float32 [256, 2048], P('feat', 'dom')
The draws below stay inside these ranges and needn't reach their ends.
Inputs may be any that keep to these rules, and one draw needn't show every extreme that they name: `want_rows`: slots at or beyond live_counts[r, o] are ignored. `live_counts`: in every draw a quarter of the owners, every fourth one from a drawn offset, receive all 128 slots from every requester. `hop_one`: each entry is o * 128 + c, a position in the buffer of the requester that holds seed s, with c < live_counts of that requester and owner o. `hop_two`: each entry is o * 128 + c, a position in the buffer of the requester that holds seed s, with c < live_counts of that requester and owner o.
All inputs are finite; a program needn't handle non-finite values.
Results may differ from the reference program's by a relative error of at most 0.00036.
Values may be sent and summed in bfloat16 or wider, within the bound.
A program may use at most 64 MiB of HBM per device.

```python
import jax
import jax.numpy as jnp
from jax import lax

FEAT = 128
HID = 256
OUT = 256
FAN1 = 15
FAN2 = 10
CAP = 128
SEED_DEV = 256
NODE_DEV = 16384
OWNERS = 8
SEEDS = 2048
NODES = 131072


def slot_plan(key):
    offset = jax.random.randint(jax.random.fold_in(key, 501), (), 0, 4)
    owner = jnp.arange(OWNERS, dtype=jnp.int32)
    spread = jax.random.randint(jax.random.fold_in(key, 502), (OWNERS, OWNERS), CAP // 8, CAP + 1)
    full = ((owner - offset) % 4 == 0)[None, :]
    return (offset, jnp.where(full, CAP, spread).astype(jnp.int32))


def positions(key, salt, lead):
    offset, counts = slot_plan(key)
    draw_key = jax.random.fold_in(key, salt)
    shape = lead + (SEEDS,)
    requester = jnp.broadcast_to(jnp.arange(SEEDS, dtype=jnp.int32) // SEED_DEV, shape)
    choose = jax.random.randint(jax.random.fold_in(draw_key, 1), shape, 0, 2)
    favored = (offset + 4 * jax.random.randint(jax.random.fold_in(draw_key, 2), shape, 0, OWNERS // 4)) % OWNERS
    anyone = jax.random.randint(jax.random.fold_in(draw_key, 3), shape, 0, OWNERS)
    owner = jnp.where(choose == 1, favored, anyone).astype(jnp.int32)
    limit = counts[requester, owner]
    slot = jax.random.randint(jax.random.fold_in(draw_key, 4), shape, 0, 1 << 20) % limit
    return (owner * CAP + slot).astype(jnp.int32)


def draw_live_counts(key, part):
    return slot_plan(key)[1]


def draw_hop_one(key, part):
    return positions(key, 11, (FAN1,))


def draw_hop_two(key, part):
    return positions(key, 12, (FAN2, FAN1))


def plant(values, stream_key, least, top_value):
    spot = [jax.random.randint(jax.random.fold_in(stream_key, axis), (), 0, length) for axis, length in enumerate(values.shape)]
    widest = values.shape.index(max(values.shape))
    neighbour = spot[:widest] + [(spot[widest] + 1) % values.shape[widest]] + spot[widest + 1:]
    return values.at[tuple(spot)].set(least).at[tuple(neighbour)].set(top_value)


def block_levels(rng, dims, cuts, least, top_value):
    gain = 1.0
    for axis_at, blocks in cuts:
        steps = jax.random.uniform(jax.random.fold_in(jax.random.fold_in(rng, 6), axis_at), (blocks,), jnp.float32, least / len(cuts), top_value / len(cuts))
        gain = gain * jnp.repeat(jnp.exp(steps), dims[axis_at] // blocks).reshape((-1,) + (1,) * (len(dims) - 1 - axis_at))
    return gain


def centred(own_key, dims, scale, most, pieces=(), kind=jnp.bfloat16):
    level = block_levels(own_key, dims, pieces, -0.22, 0.18) if pieces else 1.0
    entries = jax.random.normal(own_key, dims, jnp.float32) * scale * level
    return jnp.minimum(jnp.maximum(entries, -most), most).astype(kind)


def setup_inputs(seed: int = 0) -> dict:
    arg_keys = jax.random.split(jax.random.key(seed), 13)
    features = centred(arg_keys[0], (FEAT, NODES), 1.0, 6.0, ((0, 4), (1, 8)))
    seed_rows = plant(jax.random.randint(arg_keys[1], (SEEDS,), 0, NODE_DEV), jax.random.fold_in(arg_keys[1], 1), 0, NODE_DEV - 1).astype(jnp.int32)
    want_rows = plant(jax.random.randint(arg_keys[2], (OWNERS, OWNERS, CAP), 0, NODE_DEV), jax.random.fold_in(arg_keys[2], 1), 0, NODE_DEV - 1).astype(jnp.int32)
    live_counts = draw_live_counts(jax.random.fold_in(arg_keys[12], 71), 0)
    hop_one = draw_hop_one(jax.random.fold_in(arg_keys[12], 71), 0)
    hop_two = draw_hop_two(jax.random.fold_in(arg_keys[12], 71), 0)
    w1_self = centred(arg_keys[6], (HID, FEAT), FEAT ** -0.5, 0.5)
    w1_neigh = centred(arg_keys[7], (HID, FEAT), FEAT ** -0.5, 0.5)
    b1 = centred(arg_keys[8], (HID,), 1.0, 4.0, ((0, 4),), jnp.float32)
    w2_self = centred(arg_keys[9], (OUT, HID), HID ** -0.5, 0.375, ((1, 4),))
    w2_neigh = centred(arg_keys[10], (OUT, HID), HID ** -0.5, 0.375, ((1, 4),))
    b2 = centred(arg_keys[11], (OUT,), 1.0, 4.0, ((0, 4),), jnp.float32)
    return {"features": features, "seed_rows": seed_rows, "want_rows": want_rows, "live_counts": live_counts, "hop_one": hop_one, "hop_two": hop_two, "w1_self": w1_self, "w1_neigh": w1_neigh, "b1": b1, "w2_self": w2_self, "w2_neigh": w2_neigh, "b2": b2}


def reference(features, seed_rows, want_rows, live_counts, hop_one, hop_two, w1_self, w1_neigh, b1, w2_self, w2_neigh, b2):
    owner = jnp.arange(OWNERS, dtype=jnp.int32)
    nodes = want_rows + (owner * NODE_DEV)[None, :, None]
    fetched = jnp.take(features, nodes.reshape(-1).astype(jnp.int32), axis=1)
    slot = jnp.arange(CAP, dtype=jnp.int32)
    live = slot[None, None, :] < live_counts[:, :, None]
    fetched = jnp.where(live.reshape(1, -1), fetched, jnp.zeros((), fetched.dtype))
    requester = jnp.arange(SEEDS, dtype=jnp.int32) // SEED_DEV
    base = requester * (OWNERS * CAP)
    x_one = jnp.take(fetched, (hop_one + base[None, :]).reshape(-1).astype(jnp.int32), axis=1)

    def add_hop(number, total):
        picked = jnp.take(fetched, (hop_two[number] + base[None, :]).reshape(-1).astype(jnp.int32), axis=1)
        return total + picked.astype(jnp.float32)
    m_two = lax.fori_loop(0, FAN2, add_hop, jnp.zeros((FEAT, FAN1 * SEEDS), jnp.float32))
    m_two = (m_two * (1.0 / FAN2)).astype(jnp.bfloat16)
    x_seed = jnp.take(features, (seed_rows + requester * NODE_DEV).astype(jnp.int32), axis=1)
    m_one = (lax.optimization_barrier(jnp.sum(x_one.reshape(FEAT, FAN1, SEEDS).astype(jnp.float32), axis=1)) * (1.0 / FAN1)).astype(jnp.bfloat16)

    def layer(selves, means):
        pre = jnp.dot(w1_self, selves, preferred_element_type=jnp.float32)
        pre = pre + jnp.dot(w1_neigh, means, preferred_element_type=jnp.float32) + b1[:, None]
        return jnp.maximum(pre, 0.0)
    h_one = layer(x_one, m_two)
    h_seed = layer(x_seed, m_one)
    g_mean = lax.optimization_barrier(jnp.sum(h_one.reshape(HID, FAN1, SEEDS), axis=1)) * (1.0 / FAN1)
    z_out = jnp.dot(w2_self.astype(jnp.float32), h_seed, precision=lax.Precision.HIGHEST, preferred_element_type=jnp.float32)
    z_out = z_out + jnp.dot(w2_neigh.astype(jnp.float32), g_mean, precision=lax.Precision.HIGHEST, preferred_element_type=jnp.float32) + b2[:, None]
    square = lax.optimization_barrier(jnp.sum(z_out * z_out, axis=0))
    return z_out * lax.rsqrt(square * (1.0 / OUT) + 1.0)
```

```python
import functools

import jax
import jax.numpy as jnp
from jax import lax
from jax.experimental import pallas as pl
from jax.experimental.pallas import tpu as pltpu
from jax.sharding import PartitionSpec as P

LANES = 128
MESH = pl.DeviceIdType.MESH
BF16 = jnp.bfloat16
F32 = jnp.float32


def gather_columns(feat_vm, rows):
    height, nodes = feat_vm.shape
    shape = (height, LANES)
    high = [jnp.broadcast_to(r >> 7, shape) for r in rows]
    low = [jnp.broadcast_to(r & (LANES - 1), shape) for r in rows]
    step = 4

    def body(i, accs):
        for u in range(step):
            t = i * step + u
            start = pl.multiple_of(t * LANES, LANES)
            tile = feat_vm[:, pl.ds(start, LANES)].astype(F32)
            accs = tuple(
                jnp.where(
                    h == t,
                    jnp.take_along_axis(tile, l, axis=1, mode="promise_in_bounds"),
                    a,
                )
                for a, h, l in zip(accs, high, low)
            )
        return accs

    init = tuple(jnp.zeros(shape, F32) for _ in rows)
    return lax.fori_loop(0, nodes // LANES // step, body, init)


def split_three(x):
    a = x.astype(BF16)
    rest = x - a.astype(F32)
    b = rest.astype(BF16)
    c = (rest - b.astype(F32)).astype(BF16)
    return a, b, c


def kernel(
    nd,
    nf,
    feat_hbm,
    seed_ref,
    want_ref,
    live_ref,
    one_ref,
    two_ref,
    w1s_ref,
    w1n_ref,
    w2_ref,
    bias_ref,
    out_ref,
    feat_vm,
    got,
    served,
    back,
    everyone,
    seed_own,
    seed_all,
    w2_all,
    bias_all,
    hop_rows,
    pick_one,
    pick_two,
    fetched,
    x_all,
    m_all,
    w2_full,
    z_own,
    z_all,
    local_sem,
    want_send,
    want_recv,
    serve_send,
    serve_recv,
    all_send,
    all_recv,
    seed_send,
    seed_recv,
    w2_send,
    w2_recv,
    bias_send,
    bias_recv,
    z_send,
    z_recv,
):
    height = feat_vm.shape[0]
    fan1, seeds = one_ref.shape
    fan2 = two_ref.shape[0]
    sub = seeds // nf
    per = LANES // sub
    chunks = (fan1 + 1) * sub // LANES
    hid_dev = out_ref.shape[0]
    hid = w1s_ref.shape[0]
    depth = w1s_ref.shape[1]
    me = lax.axis_index("dom")
    mf = lax.axis_index("feat")

    def dom_at(d):
        return lax.rem(me + d, nd)

    def feat_at(d):
        return lax.rem(mf + d, nf)

    feat_copy = pltpu.make_async_copy(feat_hbm, feat_vm, local_sem)
    feat_copy.start()

    barrier = pltpu.get_barrier_semaphore()
    for d in range(1, nd):
        pl.semaphore_signal(barrier, inc=1, device_id={"dom": dom_at(d)}, device_id_type=MESH)
    for d in range(1, nf):
        pl.semaphore_signal(barrier, inc=1, device_id={"feat": feat_at(d)}, device_id_type=MESH)
    pl.semaphore_wait(barrier, nd + nf - 2)

    def remote(src, dst, send, recv, where):
        copy = pltpu.make_async_remote_copy(
            src_ref=src,
            dst_ref=dst,
            send_sem=send,
            recv_sem=recv,
            device_id=where,
            device_id_type=MESH,
        )
        copy.start()
        return copy

    wants = [
        remote(want_ref.at[0], got.at[me], want_send.at[d], want_recv.at[d], {"dom": dom_at(d)})
        for d in range(1, nd)
    ]
    early = []
    for d in range(1, nf):
        where = {"feat": feat_at(d)}
        early.append(remote(bias_ref, bias_all.at[mf], bias_send.at[d], bias_recv.at[d], where))
        early.append(remote(w2_ref, w2_all.at[mf], w2_send.at[d], w2_recv.at[d], where))
    got[me] = want_ref[0]
    bias_all[mf] = bias_ref[...]
    w2_all[mf] = w2_ref[...]

    feat_copy.wait()
    groups = seeds // LANES
    for g, block in enumerate(
        gather_columns(feat_vm, [seed_ref[:, g * LANES : (g + 1) * LANES] for g in range(groups)])
    ):
        seed_own[g] = block.astype(BF16)
    seed_copies = [
        remote(
            seed_own.at[feat_at(d) * sub // LANES],
            seed_all.at[mf],
            seed_send.at[d],
            seed_recv.at[d],
            {"feat": feat_at(d)},
        )
        for d in range(1, nf)
    ]
    seed_all[mf] = seed_own[mf * sub // LANES]

    for copy in wants:
        copy.wait_recv()

    serves = []
    order = list(range(1, nd)) + [0]
    for first in range(0, nd, 4):
        part = order[first : first + 4]
        blocks = gather_columns(feat_vm, [got[dom_at(d), pl.ds(me, 1), :] for d in part])
        for d, block in zip(part, blocks):
            if d == 0:
                back[me] = block.astype(BF16)
                continue
            served[d] = block.astype(BF16)
            serves.append(
                remote(
                    served.at[d],
                    back.at[me],
                    serve_send.at[d],
                    serve_recv.at[d],
                    {"dom": dom_at(d)},
                )
            )

    lane = lax.broadcasted_iota(jnp.int32, (1, LANES), 1)
    base = pl.multiple_of(mf * sub // LANES * LANES, LANES)
    within = lax.rem(mf * sub, LANES)
    for k in range(fan2 + 1):
        if k < fan2:
            rows = two_ref[k, :, pl.ds(base, LANES)]
        else:
            rows = one_ref[:, pl.ds(base, LANES)]
        turned = [
            pltpu.roll(rows, lax.rem(q * sub - within + LANES, LANES), 1) for q in range(per)
        ]
        for c in range(chunks):
            row = jnp.full((1, LANES), -1, jnp.int32)
            for q in range(per):
                j = c * per + q
                if j < fan1:
                    inside = (lane >= q * sub) & (lane < (q + 1) * sub)
                    row = jnp.where(inside, turned[q][j : j + 1], row)
            hop_rows[c, k : k + 1, :] = row

    slot = lax.broadcasted_iota(jnp.int32, (LANES, LANES), 0)

    def build(o, carry):
        start = pl.multiple_of(o * LANES, LANES)
        place = slot + o * LANES
        for c in range(chunks):
            columns = slice(c * LANES, (c + 1) * LANES)
            count = jnp.zeros((LANES, LANES), F32)
            for k in range(fan2):
                count = count + jnp.where(hop_rows[c, k : k + 1, :] == place, 1.0, 0.0)
            pick_two[pl.ds(start, LANES), columns] = count.astype(BF16)
            pick_one[pl.ds(start, LANES), columns] = jnp.where(
                hop_rows[c, fan2 : fan2 + 1, :] == place, 1.0, 0.0
            ).astype(BF16)
        return carry

    half = nd // 2
    lax.fori_loop(0, half, build, 0)

    for copy in serves:
        copy.wait_recv()
    everyone_copies = [
        remote(back, everyone.at[mf], all_send.at[d], all_recv.at[d], {"feat": feat_at(d)})
        for d in range(1, nf)
    ]
    everyone[mf] = back[...]

    lax.fori_loop(half, nd, build, 0)

    for copy in early:
        copy.wait_recv()
    w2_full[...] = jnp.concatenate(
        [w2_all[f, :, :hid_dev] for f in range(nf)]
        + [w2_all[f, :, hid_dev : 2 * hid_dev] for f in range(nf)],
        axis=1,
    )
    turned = [
        jnp.transpose(jnp.broadcast_to(bias_all[f], (LANES, bias_all.shape[2]))) for f in range(nf)
    ]
    b1 = jnp.concatenate([t[:hid_dev] for t in turned], axis=0)
    b2 = jnp.concatenate([t[hid_dev : 2 * hid_dev] for t in turned], axis=0)
    for copy in seed_copies:
        copy.wait_recv()
    if height % 16:
        x_seed = seed_all[...].astype(F32).reshape(depth, LANES)
    else:
        x_seed = seed_all[...].reshape(depth, LANES).astype(F32)
    x_seed = pltpu.roll(x_seed, lax.rem(2 * LANES - sub - within, LANES), 1)

    for copy in everyone_copies:
        copy.wait_recv()
    for o in range(nd):
        live = lane < live_ref[0, o]
        if height % 16:
            block = everyone[:, o].astype(F32).reshape(depth, LANES)
        else:
            block = everyone[:, o].reshape(depth, LANES).astype(F32)
        fetched[:, o * LANES : (o + 1) * LANES] = jnp.where(live, block, 0.0).astype(BF16)

    wide = 2 * LANES
    total = jnp.zeros((depth, LANES), F32)
    for n in range(chunks * LANES // wide):
        columns = slice(n * wide, (n + 1) * wide)
        own = jnp.dot(fetched[...], pick_one[:, columns], preferred_element_type=F32)
        mean = jnp.dot(fetched[...], pick_two[:, columns], preferred_element_type=F32)
        total = total + own[:, :LANES] + own[:, LANES:]
        x_all[:, columns] = own.astype(BF16)
        m_all[:, columns] = (mean * (1.0 / fan2)).astype(BF16)

    def fold(value):
        width = sub
        while width < LANES:
            value = value + pltpu.roll(value, width, 1)
            width *= 2
        return value

    is_seed = lane >= LANES - sub
    last = slice((chunks - 1) * LANES, chunks * LANES)
    m_one = fold(total) * (1.0 / fan1)
    x_all[:, last] = jnp.where(is_seed, x_seed, x_all[:, last].astype(F32)).astype(BF16)
    m_all[:, last] = jnp.where(is_seed, m_one, m_all[:, last].astype(F32)).astype(BF16)

    total = jnp.zeros((hid, LANES), F32)
    for n in range(chunks * LANES // wide):
        columns = slice(n * wide, (n + 1) * wide)
        pre = jnp.dot(w1s_ref[...], x_all[:, columns], preferred_element_type=F32)
        pre = pre + jnp.dot(w1n_ref[...], m_all[:, columns], preferred_element_type=F32)
        left = jnp.maximum(pre[:, :LANES] + b1, 0.0)
        right = jnp.maximum(pre[:, LANES:] + b1, 0.0)
        if n == chunks * LANES // wide - 1:
            h_seed = right
            right = jnp.where(is_seed, 0.0, right)
        total = total + left + right
    g_mean = fold(total) * (1.0 / fan1)
    stacked = jnp.concatenate([h_seed, g_mean], axis=0)
    z = jnp.zeros((hid, LANES), F32)
    for term in reversed(split_three(stacked)):
        z = z + jnp.dot(w2_full[...], term, preferred_element_type=F32)
    z = z + b2
    square = jnp.sum(z * z, axis=0, keepdims=True)
    z = z * lax.rsqrt(square * (1.0 / hid) + 1.0)
    for f in range(nf):
        z_own[f] = z[f * hid_dev : (f + 1) * hid_dev]

    z_copies = [
        remote(
            z_own.at[feat_at(d)],
            z_all.at[mf],
            z_send.at[d],
            z_recv.at[d],
            {"feat": feat_at(d)},
        )
        for d in range(1, nf)
    ]
    z_all[mf] = z_own[mf]
    for copy in wants + early + seed_copies + serves + everyone_copies:
        copy.wait_send()
    for copy in z_copies:
        copy.wait_recv()
    for g in range(groups):
        block = jnp.zeros((hid_dev, LANES), F32)
        for q in range(per):
            value = z_all[g * per + q]
            shift = (q * sub + sub) % LANES
            if shift:
                value = pltpu.roll(value, shift, 1)
            inside = (lane >= q * sub) & (lane < (q + 1) * sub)
            block = jnp.where(inside, value, block)
        out_ref[:, g * LANES : (g + 1) * LANES] = block
    for copy in z_copies:
        copy.wait_send()


def per_device(
    nd,
    nf,
    features,
    seed_rows,
    want_rows,
    live_counts,
    hop_one,
    hop_two,
    w1_self,
    w1_neigh,
    b1,
    w2_self,
    w2_neigh,
    b2,
):
    height, nodes = features.shape
    seeds = seed_rows.shape[0]
    hid_dev = b1.shape[0]
    hid, depth = w1_self.shape
    cap = want_rows.shape[2]
    fan1 = hop_one.shape[0]
    fan2 = hop_two.shape[0]
    columns = (fan1 + 1) * (seeds // nf)
    w2 = jnp.concatenate([w2_self, w2_neigh], axis=1)
    bias = jnp.concatenate([b1, b2]).reshape(1, 2 * hid_dev)
    vmem = pl.BlockSpec(memory_space=pltpu.VMEM)
    dma = pltpu.SemaphoreType.DMA
    return pl.pallas_call(
        functools.partial(kernel, nd, nf),
        out_shape=jax.ShapeDtypeStruct((hid_dev, seeds), F32),
        in_specs=[
            pl.BlockSpec(memory_space=pl.ANY),
            vmem,
            vmem,
            pl.BlockSpec(memory_space=pltpu.SMEM),
        ]
        + [vmem] * 6,
        out_specs=vmem,
        scratch_shapes=[
            pltpu.VMEM((height, nodes), BF16),
            pltpu.VMEM((nd, nd, cap), jnp.int32),
            pltpu.VMEM((nd, height, cap), BF16),
            pltpu.VMEM((nd, height, cap), BF16),
            pltpu.VMEM((nf, nd, height, cap), BF16),
            pltpu.VMEM((seeds // LANES, height, LANES), BF16),
            pltpu.VMEM((nf, height, LANES), BF16),
            pltpu.VMEM((nf, hid, 2 * hid_dev), BF16),
            pltpu.VMEM((nf, 1, 2 * hid_dev), F32),
            pltpu.VMEM((columns // LANES, 16, LANES), jnp.int32),
            pltpu.VMEM((nd * cap, columns), BF16),
            pltpu.VMEM((nd * cap, columns), BF16),
            pltpu.VMEM((depth, nd * cap), BF16),
            pltpu.VMEM((depth, columns), BF16),
            pltpu.VMEM((depth, columns), BF16),
            pltpu.VMEM((hid, 2 * hid), BF16),
            pltpu.VMEM((nf, hid_dev, LANES), F32),
            pltpu.VMEM((nf, hid_dev, LANES), F32),
            dma,
        ]
        + [dma((nd,))] * 4
        + [dma((nf,))] * 10,
        compiler_params=pltpu.CompilerParams(collective_id=0, has_side_effects=True),
    )(
        features,
        seed_rows.reshape(1, seeds),
        want_rows,
        live_counts,
        hop_one,
        hop_two,
        w1_self,
        w1_neigh,
        w2,
        bias,
    )


def solution(mesh):
    return jax.shard_map(
        functools.partial(per_device, mesh.shape["dom"], mesh.shape["feat"]),
        mesh=mesh,
        in_specs=(
            P("feat", "dom"),
            P("dom"),
            P("dom", None, None),
            P("dom", None),
            P(None, "dom"),
            P(None, None, "dom"),
            P(),
            P(),
            P("feat"),
            P(None, "feat"),
            P(None, "feat"),
            P("feat"),
        ),
        out_specs=P("feat", "dom"),
        check_vma=False,
    )
```

```python
import functools

import jax
import jax.numpy as jnp
from jax import lax
from jax.experimental import pallas as pl
from jax.experimental.pallas import tpu as pltpu
from jax.sharding import PartitionSpec as P

LANES = 128
MESH = pl.DeviceIdType.MESH
BF16 = jnp.bfloat16
F32 = jnp.float32


def gather_columns(feat_vm, rows):
    height, nodes = feat_vm.shape
    shape = (height, LANES)
    high = [jnp.broadcast_to(r >> 7, shape) for r in rows]
    low = [jnp.broadcast_to(r & (LANES - 1), shape) for r in rows]
    step = min(32, nodes // LANES)

    def body(i, accs):
        for u in range(step):
            t = i * step + u
            start = pl.multiple_of(t * LANES, LANES)
            tile = feat_vm[:, pl.ds(start, LANES)].astype(F32)
            accs = tuple(
                jnp.where(
                    h == t,
                    jnp.take_along_axis(tile, l, axis=1, mode="promise_in_bounds"),
                    a,
                )
                for a, h, l in zip(accs, high, low)
            )
        return accs

    init = tuple(jnp.zeros(shape, F32) for _ in rows)
    return lax.fori_loop(0, nodes // LANES // step, body, init)


def split_three(x):
    a = x.astype(BF16)
    rest = x - a.astype(F32)
    b = rest.astype(BF16)
    c = (rest - b.astype(F32)).astype(BF16)
    return a, b, c


def kernel(
    nd,
    nf,
    feat_hbm,
    seed_ref,
    want_ref,
    live_ref,
    one_ref,
    two_ref,
    w1s_ref,
    w1n_ref,
    w2s_ref,
    w2n_ref,
    b1_ref,
    b2_ref,
    out_ref,
    feat_vm,
    got,
    served,
    back,
    everyone,
    seed_own,
    seed_all,
    w2_all,
    b1_all,
    b2_all,
    hop_rows,
    pick_one,
    pick_two,
    fetched,
    x_all,
    m_all,
    w2_full,
    z_own,
    z_all,
    local_sem,
    want_send,
    want_recv,
    serve_send,
    serve_recv,
    all_send,
    all_recv,
    seed_send,
    seed_recv,
    early_send,
    early_recv,
    z_send,
    z_recv,
):
    height = feat_vm.shape[0]
    fan1, seeds = one_ref.shape
    fan2 = two_ref.shape[0]
    sub = seeds // nf
    per = LANES // sub
    chunks = (fan1 + 1) * sub // LANES
    hid_dev = out_ref.shape[0]
    hid = w1s_ref.shape[0]
    depth = w1s_ref.shape[1]
    me = lax.axis_index("dom")
    mf = lax.axis_index("feat")

    def dom_at(d):
        return lax.rem(me + d, nd)

    def feat_at(d):
        return lax.rem(mf + d, nf)

    feat_copy = pltpu.make_async_copy(feat_hbm, feat_vm, local_sem)
    feat_copy.start()

    barrier = pltpu.get_barrier_semaphore()
    for d in range(1, nd):
        pl.semaphore_signal(barrier, inc=1, device_id={"dom": dom_at(d)}, device_id_type=MESH)
    for d in range(1, nf):
        pl.semaphore_signal(barrier, inc=1, device_id={"feat": feat_at(d)}, device_id_type=MESH)
    pl.semaphore_wait(barrier, nd + nf - 2)

    def remote(src, dst, send, recv, where):
        copy = pltpu.make_async_remote_copy(
            src_ref=src,
            dst_ref=dst,
            send_sem=send,
            recv_sem=recv,
            device_id=where,
            device_id_type=MESH,
        )
        copy.start()
        return copy

    wants = [
        remote(want_ref.at[0], got.at[me], want_send.at[d], want_recv.at[d], {"dom": dom_at(d)})
        for d in range(1, nd)
    ]
    early = []
    for d in range(1, nf):
        where = {"feat": feat_at(d)}
        for i, (src, dst) in enumerate(
            (
                (b1_ref, b1_all.at[mf]),
                (b2_ref, b2_all.at[mf]),
                (w2s_ref, w2_all.at[0, mf]),
                (w2n_ref, w2_all.at[1, mf]),
            )
        ):
            early.append(remote(src, dst, early_send.at[d, i], early_recv.at[d, i], where))
    got[me] = want_ref[0]
    b1_all[mf] = b1_ref[...]
    b2_all[mf] = b2_ref[...]
    w2_all[0, mf] = w2s_ref[...]
    w2_all[1, mf] = w2n_ref[...]

    feat_copy.wait()
    groups = seeds // LANES
    for g, block in enumerate(
        gather_columns(feat_vm, [seed_ref[:, g * LANES : (g + 1) * LANES] for g in range(groups)])
    ):
        seed_own[g] = block.astype(BF16)
    seed_copies = [
        remote(
            seed_own.at[feat_at(d) * sub // LANES],
            seed_all.at[mf],
            seed_send.at[d],
            seed_recv.at[d],
            {"feat": feat_at(d)},
        )
        for d in range(1, nf)
    ]
    seed_all[mf] = seed_own[mf * sub // LANES]

    for copy in wants:
        copy.wait_recv()

    def forward(part):
        copies = []
        for d in part:
            source = lax.rem(me + nd - d, nd)
            if d:
                serves[d].wait_recv()
            for e in range(1, nf):
                copies.append(
                    remote(
                        back.at[source],
                        everyone.at[mf, source],
                        all_send.at[d, e],
                        all_recv.at[d, e],
                        {"feat": feat_at(e)},
                    )
                )
            everyone[mf, source] = back[source]
        return copies

    serves = {}
    everyone_copies = []
    parts = []
    order = list(range(1, nd)) + [0]
    for first in range(0, nd, 4):
        part = order[first : first + 4]
        blocks = gather_columns(feat_vm, [got[dom_at(d), pl.ds(me, 1), :] for d in part])
        for d, block in zip(part, blocks):
            if d == 0:
                back[me] = block.astype(BF16)
                continue
            served[d] = block.astype(BF16)
            serves[d] = remote(
                served.at[d], back.at[me], serve_send.at[d], serve_recv.at[d], {"dom": dom_at(d)}
            )
        if parts:
            everyone_copies += forward(parts[-1])
        parts.append(part)

    lane = lax.broadcasted_iota(jnp.int32, (1, LANES), 1)
    base = pl.multiple_of(mf * sub // LANES * LANES, LANES)
    within = lax.rem(mf * sub, LANES)
    for k in range(fan2 + 1):
        if k < fan2:
            rows = two_ref[k, :, pl.ds(base, LANES)]
        else:
            rows = one_ref[:, pl.ds(base, LANES)]
        turned = [
            pltpu.roll(rows, lax.rem(q * sub - within + LANES, LANES), 1) for q in range(per)
        ]
        for c in range(chunks):
            row = jnp.full((1, LANES), -1, jnp.int32)
            for q in range(per):
                j = c * per + q
                if j < fan1:
                    inside = (lane >= q * sub) & (lane < (q + 1) * sub)
                    row = jnp.where(inside, turned[q][j : j + 1], row)
            hop_rows[c, k : k + 1, :] = row

    slot = lax.broadcasted_iota(jnp.int32, (LANES, LANES), 0)

    def build(o, carry):
        start = pl.multiple_of(o * LANES, LANES)
        place = slot + o * LANES
        for c in range(chunks):
            columns = slice(c * LANES, (c + 1) * LANES)
            count = jnp.zeros((LANES, LANES), F32)
            for k in range(fan2):
                count = count + jnp.where(hop_rows[c, k : k + 1, :] == place, 1.0, 0.0)
            pick_two[pl.ds(start, LANES), columns] = count.astype(BF16)
            pick_one[pl.ds(start, LANES), columns] = jnp.where(
                hop_rows[c, fan2 : fan2 + 1, :] == place, 1.0, 0.0
            ).astype(BF16)
        return carry

    half = nd // 2
    lax.fori_loop(0, half, build, 0)

    everyone_copies += forward(parts[-1])

    lax.fori_loop(half, nd, build, 0)

    for copy in early:
        copy.wait_recv()
    w2_full[...] = jnp.transpose(w2_all[...].reshape(2 * hid, w2_all.shape[3]))

    def column(rows):
        return jnp.concatenate(
            [jnp.transpose(jnp.broadcast_to(rows[f], (LANES, hid_dev))) for f in range(nf)], axis=0
        )

    b1 = column(b1_all)
    b2 = column(b2_all)
    for copy in seed_copies:
        copy.wait_recv()
    if height % 16:
        x_seed = seed_all[...].astype(F32).reshape(depth, LANES)
    else:
        x_seed = seed_all[...].reshape(depth, LANES).astype(F32)
    x_seed = pltpu.roll(x_seed, lax.rem(2 * LANES - sub - within, LANES), 1)

    for copy in everyone_copies:
        copy.wait_recv()
    for o in range(nd):
        live = lane < live_ref[0, o]
        if height % 16:
            block = everyone[:, o].astype(F32).reshape(depth, LANES)
        else:
            block = everyone[:, o].reshape(depth, LANES).astype(F32)
        fetched[:, o * LANES : (o + 1) * LANES] = jnp.where(live, block, 0.0).astype(BF16)

    wide = 2 * LANES
    total = jnp.zeros((depth, LANES), F32)
    for n in range(chunks * LANES // wide):
        columns = slice(n * wide, (n + 1) * wide)
        own = jnp.dot(fetched[...], pick_one[:, columns], preferred_element_type=F32)
        mean = jnp.dot(fetched[...], pick_two[:, columns], preferred_element_type=F32)
        total = total + own[:, :LANES] + own[:, LANES:]
        x_all[:, columns] = own.astype(BF16)
        m_all[:, columns] = (mean * (1.0 / fan2)).astype(BF16)

    def fold(value):
        width = sub
        while width < LANES:
            value = value + pltpu.roll(value, width, 1)
            width *= 2
        return value

    is_seed = lane >= LANES - sub
    last = slice((chunks - 1) * LANES, chunks * LANES)
    m_one = fold(total) * (1.0 / fan1)
    x_all[:, last] = jnp.where(is_seed, x_seed, x_all[:, last].astype(F32)).astype(BF16)
    m_all[:, last] = jnp.where(is_seed, m_one, m_all[:, last].astype(F32)).astype(BF16)

    total = jnp.zeros((hid, LANES), F32)
    for n in range(chunks * LANES // wide):
        columns = slice(n * wide, (n + 1) * wide)
        pre = jnp.dot(w1s_ref[...], x_all[:, columns], preferred_element_type=F32)
        pre = pre + jnp.dot(w1n_ref[...], m_all[:, columns], preferred_element_type=F32)
        left = jnp.maximum(pre[:, :LANES] + b1, 0.0)
        right = jnp.maximum(pre[:, LANES:] + b1, 0.0)
        if n == chunks * LANES // wide - 1:
            h_seed = right
            right = jnp.where(is_seed, 0.0, right)
        total = total + left + right
    g_mean = fold(total) * (1.0 / fan1)
    stacked = jnp.concatenate([h_seed, g_mean], axis=0)
    z = jnp.zeros((hid, LANES), F32)
    for term in reversed(split_three(stacked)):
        z = z + jnp.dot(w2_full[...], term, preferred_element_type=F32)
    z = z + b2
    square = jnp.sum(z * z, axis=0, keepdims=True)
    z = z * lax.rsqrt(square * (1.0 / hid) + 1.0)
    part_rows = hid_dev // per
    for f in range(nf):
        packed = jnp.zeros((part_rows, LANES), F32)
        for p in range(per):
            row = f * hid_dev + p * part_rows
            value = z[row : row + part_rows]
            shift = (p * sub + sub) % LANES
            if shift:
                value = pltpu.roll(value, shift, 1)
            packed = jnp.where((lane >= p * sub) & (lane < (p + 1) * sub), value, packed)
        z_own[f] = packed

    z_copies = [
        remote(
            z_own.at[feat_at(d)],
            z_all.at[mf],
            z_send.at[d],
            z_recv.at[d],
            {"feat": feat_at(d)},
        )
        for d in range(1, nf)
    ]
    z_all[mf] = z_own[mf]
    for copy in wants + early + seed_copies + list(serves.values()) + everyone_copies:
        copy.wait_send()
    for copy in z_copies:
        copy.wait_recv()
    for g in range(groups):
        for p in range(per):
            block = jnp.zeros((part_rows, LANES), F32)
            for q in range(per):
                value = z_all[g * per + q]
                shift = (q - p) * sub % LANES
                if shift:
                    value = pltpu.roll(value, shift, 1)
                inside = (lane >= q * sub) & (lane < (q + 1) * sub)
                block = jnp.where(inside, value, block)
            out_ref[p * part_rows : (p + 1) * part_rows, g * LANES : (g + 1) * LANES] = block
    for copy in z_copies:
        copy.wait_send()


def per_device(
    nd,
    nf,
    features,
    seed_rows,
    want_rows,
    live_counts,
    hop_one,
    hop_two,
    w1_self,
    w1_neigh,
    b1,
    w2_self,
    w2_neigh,
    b2,
):
    height, nodes = features.shape
    seeds = seed_rows.shape[0]
    hid_dev = b1.shape[0]
    hid, depth = w1_self.shape
    cap = want_rows.shape[2]
    fan1 = hop_one.shape[0]
    fan2 = hop_two.shape[0]
    columns = (fan1 + 1) * (seeds // nf)
    vmem = pl.BlockSpec(memory_space=pltpu.VMEM)
    dma = pltpu.SemaphoreType.DMA
    return pl.pallas_call(
        functools.partial(kernel, nd, nf),
        out_shape=pltpu.VMEM((hid_dev, seeds), F32),
        in_specs=[
            pl.BlockSpec(memory_space=pl.ANY),
            vmem,
            vmem,
            pl.BlockSpec(memory_space=pltpu.SMEM),
        ]
        + [vmem] * 8,
        out_specs=vmem,
        scratch_shapes=[
            pltpu.VMEM((height, nodes), BF16),
            pltpu.VMEM((nd, nd, cap), jnp.int32),
            pltpu.VMEM((nd, height, cap), BF16),
            pltpu.VMEM((nd, height, cap), BF16),
            pltpu.VMEM((nf, nd, height, cap), BF16),
            pltpu.VMEM((seeds // LANES, height, LANES), BF16),
            pltpu.VMEM((nf, height, LANES), BF16),
            pltpu.VMEM((2, nf, hid_dev, w2_self.shape[0]), BF16),
            pltpu.VMEM((nf, 1, hid_dev), F32),
            pltpu.VMEM((nf, 1, hid_dev), F32),
            pltpu.VMEM((columns // LANES, 16, LANES), jnp.int32),
            pltpu.VMEM((nd * cap, columns), BF16),
            pltpu.VMEM((nd * cap, columns), BF16),
            pltpu.VMEM((depth, nd * cap), BF16),
            pltpu.VMEM((depth, columns), BF16),
            pltpu.VMEM((depth, columns), BF16),
            pltpu.VMEM((hid, 2 * hid), BF16),
            pltpu.VMEM((nf, hid_dev * (seeds // nf) // LANES, LANES), F32),
            pltpu.VMEM((nf, hid_dev * (seeds // nf) // LANES, LANES), F32),
            dma,
        ]
        + [dma((nd,))] * 4
        + [dma((nd, nf))] * 2
        + [dma((nf,))] * 2
        + [dma((nf, 4))] * 2
        + [dma((nf,))] * 2,
        compiler_params=pltpu.CompilerParams(collective_id=0, has_side_effects=True),
    )(
        features,
        seed_rows.reshape(1, seeds),
        want_rows,
        live_counts,
        hop_one,
        hop_two,
        w1_self,
        w1_neigh,
        w2_self.T,
        w2_neigh.T,
        b1.reshape(1, hid_dev),
        b2.reshape(1, hid_dev),
    )


def solution(mesh):
    return jax.shard_map(
        functools.partial(per_device, mesh.shape["dom"], mesh.shape["feat"]),
        mesh=mesh,
        in_specs=(
            P("feat", "dom"),
            P("dom"),
            P("dom", None, None),
            P("dom", None),
            P(None, "dom"),
            P(None, None, "dom"),
            P(),
            P(),
            P("feat"),
            P(None, "feat"),
            P(None, "feat"),
            P("feat"),
        ),
        out_specs=P("feat", "dom"),
        check_vma=False,
    )
```

```python
import functools

import jax
import jax.numpy as jnp
from jax import lax
from jax.experimental import pallas as pl
from jax.experimental.pallas import tpu as pltpu
from jax.sharding import PartitionSpec as P

LANES = 128
MESH = pl.DeviceIdType.MESH
BF16 = jnp.bfloat16
F32 = jnp.float32


def gather_columns(feat_vm, rows):
    height, nodes = feat_vm.shape
    shape = (height, LANES)
    high = [jnp.broadcast_to(r >> 7, shape) for r in rows]
    low = [jnp.broadcast_to(r & (LANES - 1), shape) for r in rows]
    step = min(32, nodes // LANES)

    def body(i, accs):
        for u in range(step):
            t = i * step + u
            start = pl.multiple_of(t * LANES, LANES)
            tile = feat_vm[:, pl.ds(start, LANES)].astype(F32)
            accs = tuple(
                jnp.where(
                    h == t,
                    jnp.take_along_axis(tile, l, axis=1, mode="promise_in_bounds"),
                    a,
                )
                for a, h, l in zip(accs, high, low)
            )
        return accs

    init = tuple(jnp.zeros(shape, F32) for _ in rows)
    return lax.fori_loop(0, nodes // LANES // step, body, init)


def split_three(x):
    a = x.astype(BF16)
    rest = x - a.astype(F32)
    b = rest.astype(BF16)
    c = (rest - b.astype(F32)).astype(BF16)
    return a, b, c


def kernel(
    nd,
    nf,
    feat_hbm,
    seed_ref,
    want_ref,
    live_ref,
    one_hbm,
    two_hbm,
    w1s_hbm,
    w1n_hbm,
    w2s_ref,
    w2n_ref,
    b1_ref,
    b2_ref,
    out_ref,
    feat_vm,
    one_ref,
    two_ref,
    w1s_ref,
    w1n_ref,
    got,
    served,
    back,
    everyone,
    seed_own,
    seed_all,
    w2_all,
    b1_all,
    b2_all,
    hop_rows,
    pick_one,
    pick_two,
    fetched,
    own_sum,
    mean_sum,
    x_all,
    m_all,
    w2_full,
    z_own,
    z_all,
    local_sem,
    want_send,
    want_recv,
    serve_send,
    serve_recv,
    all_send,
    all_recv,
    seed_send,
    seed_recv,
    early_send,
    early_recv,
    z_send,
    z_recv,
):
    height = feat_vm.shape[0]
    fan1, seeds = one_ref.shape
    fan2 = two_ref.shape[0]
    sub = seeds // nf
    per = LANES // sub
    chunks = (fan1 + 1) * sub // LANES
    hid_dev = out_ref.shape[0]
    hid = w1s_ref.shape[0]
    depth = w1s_ref.shape[1]
    me = lax.axis_index("dom")
    mf = lax.axis_index("feat")

    def dom_at(d):
        return lax.rem(me + d, nd)

    def feat_at(d):
        return lax.rem(mf + d, nf)

    feat_copy = pltpu.make_async_copy(feat_hbm, feat_vm, local_sem.at[0])
    feat_copy.start()
    hop_copies = [
        pltpu.make_async_copy(one_hbm, one_ref, local_sem.at[1]),
        pltpu.make_async_copy(two_hbm, two_ref, local_sem.at[2]),
    ]
    weight_copies = [
        pltpu.make_async_copy(w1s_hbm, w1s_ref, local_sem.at[3]),
        pltpu.make_async_copy(w1n_hbm, w1n_ref, local_sem.at[4]),
        pltpu.make_async_copy(w2s_ref, w2_all.at[0, mf], local_sem.at[5]),
        pltpu.make_async_copy(w2n_ref, w2_all.at[1, mf], local_sem.at[6]),
    ]

    barrier = pltpu.get_barrier_semaphore()
    for d in range(1, nd):
        pl.semaphore_signal(barrier, inc=1, device_id={"dom": dom_at(d)}, device_id_type=MESH)
    for d in range(1, nf):
        pl.semaphore_signal(barrier, inc=1, device_id={"feat": feat_at(d)}, device_id_type=MESH)
    pl.semaphore_wait(barrier, nd + nf - 2)

    def remote(src, dst, send, recv, where):
        copy = pltpu.make_async_remote_copy(
            src_ref=src,
            dst_ref=dst,
            send_sem=send,
            recv_sem=recv,
            device_id=where,
            device_id_type=MESH,
        )
        copy.start()
        return copy

    wants = [
        remote(want_ref.at[0], got.at[me], want_send.at[d], want_recv.at[d], {"dom": dom_at(d)})
        for d in range(1, nd)
    ]
    early = []
    for d in range(1, nf):
        where = {"feat": feat_at(d)}
        for i, (src, dst) in enumerate(
            (
                (b1_ref, b1_all.at[mf]),
                (b2_ref, b2_all.at[mf]),
                (w2s_ref, w2_all.at[0, mf]),
                (w2n_ref, w2_all.at[1, mf]),
            )
        ):
            early.append(remote(src, dst, early_send.at[d, i], early_recv.at[d, i], where))
    got[me] = want_ref[0]
    b1_all[mf] = b1_ref[...]
    b2_all[mf] = b2_ref[...]
    for copy in hop_copies + weight_copies:
        copy.start()

    feat_copy.wait()
    groups = seeds // LANES
    for g, block in enumerate(
        gather_columns(feat_vm, [seed_ref[:, g * LANES : (g + 1) * LANES] for g in range(groups)])
    ):
        seed_own[g] = block.astype(BF16)
    seed_copies = [
        remote(
            seed_own.at[feat_at(d) * sub // LANES],
            seed_all.at[mf],
            seed_send.at[d],
            seed_recv.at[d],
            {"feat": feat_at(d)},
        )
        for d in range(1, nf)
    ]
    seed_all[mf] = seed_own[mf * sub // LANES]

    for copy in wants:
        copy.wait_recv()

    def forward(part):
        copies = []
        for d in part:
            source = lax.rem(me + nd - d, nd)
            if d:
                serves[d].wait_recv()
            for e in range(1, nf):
                copies.append(
                    remote(
                        back.at[source],
                        everyone.at[mf, source],
                        all_send.at[d, e],
                        all_recv.at[d, e],
                        {"feat": feat_at(e)},
                    )
                )
            everyone[mf, source] = back[source]
        return copies

    serves = {}
    arrivals = []
    parts = []
    order = list(range(1, nd)) + [0]
    for part in (order[: nd * 3 // 8], order[nd * 3 // 8 : nd * 6 // 8], order[nd * 6 // 8 :]):
        blocks = gather_columns(feat_vm, [got[dom_at(d), pl.ds(me, 1), :] for d in part])
        for d, block in zip(part, blocks):
            if d == 0:
                back[me] = block.astype(BF16)
                continue
            served[d] = block.astype(BF16)
            serves[d] = remote(
                served.at[d], back.at[me], serve_send.at[d], serve_recv.at[d], {"dom": dom_at(d)}
            )
        if parts:
            arrivals.append(forward(parts[-1]))
        parts.append(part)

    lane = lax.broadcasted_iota(jnp.int32, (1, LANES), 1)
    base = pl.multiple_of(mf * sub // LANES * LANES, LANES)
    within = lax.rem(mf * sub, LANES)
    for copy in hop_copies:
        copy.wait()
    for k in range(fan2 + 1):
        if k < fan2:
            rows = two_ref[k, :, pl.ds(base, LANES)]
        else:
            rows = one_ref[:, pl.ds(base, LANES)]
        turned = [
            pltpu.roll(rows, lax.rem(q * sub - within + LANES, LANES), 1) for q in range(per)
        ]
        for c in range(chunks):
            row = jnp.full((1, LANES), -1, jnp.int32)
            for q in range(per):
                j = c * per + q
                if j < fan1:
                    inside = (lane >= q * sub) & (lane < (q + 1) * sub)
                    row = jnp.where(inside, turned[q][j : j + 1], row)
            hop_rows[c, k : k + 1, :] = row

    slot = lax.broadcasted_iota(jnp.int32, (LANES, LANES), 0)

    def build(o, carry):
        start = pl.multiple_of(o * LANES, LANES)
        place = slot + lax.rem(me + 2 * nd - 1 - o, nd) * LANES
        for c in range(chunks):
            columns = slice(c * LANES, (c + 1) * LANES)
            count = jnp.zeros((LANES, LANES), F32)
            for k in range(fan2):
                count = count + jnp.where(hop_rows[c, k : k + 1, :] == place, 1.0, 0.0)
            pick_two[pl.ds(start, LANES), columns] = count.astype(BF16)
            pick_one[pl.ds(start, LANES), columns] = jnp.where(
                hop_rows[c, fan2 : fan2 + 1, :] == place, 1.0, 0.0
            ).astype(BF16)
        return carry

    half = nd // 2
    lax.fori_loop(0, half, build, 0)

    arrivals.append(forward(parts[-1]))
    everyone_copies = [copy for part in arrivals for copy in part]

    lax.fori_loop(half, nd, build, 0)

    for copy in early:
        copy.wait_recv()
    for copy in weight_copies:
        copy.wait()
    w2_full[...] = jnp.transpose(w2_all[...].reshape(2 * hid, w2_all.shape[3]))

    def column(rows):
        return jnp.concatenate(
            [jnp.transpose(jnp.broadcast_to(rows[f], (LANES, hid_dev))) for f in range(nf)], axis=0
        )

    b1 = column(b1_all)
    b2 = column(b2_all)
    for copy in seed_copies:
        copy.wait_recv()
    if height % 16:
        x_seed = seed_all[...].astype(F32).reshape(depth, LANES)
    else:
        x_seed = seed_all[...].reshape(depth, LANES).astype(F32)
    x_seed = pltpu.roll(x_seed, lax.rem(2 * LANES - sub - within, LANES), 1)

    wide = 2 * LANES
    total = jnp.zeros((depth, LANES), F32)
    done = 0
    for i, part in enumerate(parts):
        for copy in arrivals[i]:
            copy.wait_recv()
        for d in part:
            source = lax.rem(me + nd - d, nd)
            live = lane < live_ref[0, source]
            if height % 16:
                block = everyone[:, source].astype(F32).reshape(depth, LANES)
            else:
                block = everyone[:, source].reshape(depth, LANES).astype(F32)
            at = order.index(d) * LANES
            fetched[:, at : at + LANES] = jnp.where(live, block, 0.0).astype(BF16)
        these = slice(done, done + len(part) * LANES)
        done += len(part) * LANES
        for n in range(chunks * LANES // wide):
            columns = slice(n * wide, (n + 1) * wide)
            own = jnp.dot(fetched[:, these], pick_one[these, columns], preferred_element_type=F32)
            mean = jnp.dot(fetched[:, these], pick_two[these, columns], preferred_element_type=F32)
            if i:
                own = own + own_sum[:, columns]
                mean = mean + mean_sum[:, columns]
            if i < len(parts) - 1:
                own_sum[:, columns] = own
                mean_sum[:, columns] = mean
                continue
            total = total + own[:, :LANES] + own[:, LANES:]
            x_all[:, columns] = own.astype(BF16)
            m_all[:, columns] = (mean * (1.0 / fan2)).astype(BF16)

    def fold(value):
        width = sub
        while width < LANES:
            value = value + pltpu.roll(value, width, 1)
            width *= 2
        return value

    is_seed = lane >= LANES - sub
    last = slice((chunks - 1) * LANES, chunks * LANES)
    m_one = fold(total) * (1.0 / fan1)
    x_all[:, last] = jnp.where(is_seed, x_seed, x_all[:, last].astype(F32)).astype(BF16)
    m_all[:, last] = jnp.where(is_seed, m_one, m_all[:, last].astype(F32)).astype(BF16)

    total = jnp.zeros((hid, LANES), F32)
    for n in range(chunks * LANES // wide):
        columns = slice(n * wide, (n + 1) * wide)
        pre = jnp.dot(w1s_ref[...], x_all[:, columns], preferred_element_type=F32)
        pre = pre + jnp.dot(w1n_ref[...], m_all[:, columns], preferred_element_type=F32)
        left = jnp.maximum(pre[:, :LANES] + b1, 0.0)
        right = jnp.maximum(pre[:, LANES:] + b1, 0.0)
        if n == chunks * LANES // wide - 1:
            h_seed = right
            right = jnp.where(is_seed, 0.0, right)
        total = total + left + right
    g_mean = fold(total) * (1.0 / fan1)
    stacked = jnp.concatenate([h_seed, g_mean], axis=0)
    z = jnp.zeros((hid, LANES), F32)
    for term in reversed(split_three(stacked)):
        z = z + jnp.dot(w2_full[...], term, preferred_element_type=F32)
    z = z + b2
    square = jnp.sum(z * z, axis=0, keepdims=True)
    z = z * lax.rsqrt(square * (1.0 / hid) + 1.0)
    part_rows = hid_dev // per
    for f in range(nf):
        packed = jnp.zeros((part_rows, LANES), F32)
        for p in range(per):
            row = f * hid_dev + p * part_rows
            value = z[row : row + part_rows]
            shift = (p * sub + sub) % LANES
            if shift:
                value = pltpu.roll(value, shift, 1)
            packed = jnp.where((lane >= p * sub) & (lane < (p + 1) * sub), value, packed)
        z_own[f] = packed

    z_copies = [
        remote(
            z_own.at[feat_at(d)],
            z_all.at[mf],
            z_send.at[d],
            z_recv.at[d],
            {"feat": feat_at(d)},
        )
        for d in range(1, nf)
    ]
    z_all[mf] = z_own[mf]
    for copy in wants + early + seed_copies + list(serves.values()) + everyone_copies:
        copy.wait_send()
    for copy in z_copies:
        copy.wait_recv()
    for g in range(groups):
        for p in range(per):
            block = jnp.zeros((part_rows, LANES), F32)
            for q in range(per):
                value = z_all[g * per + q]
                shift = (q - p) * sub % LANES
                if shift:
                    value = pltpu.roll(value, shift, 1)
                inside = (lane >= q * sub) & (lane < (q + 1) * sub)
                block = jnp.where(inside, value, block)
            out_ref[p * part_rows : (p + 1) * part_rows, g * LANES : (g + 1) * LANES] = block
    for copy in z_copies:
        copy.wait_send()


def per_device(
    nd,
    nf,
    features,
    seed_rows,
    want_rows,
    live_counts,
    hop_one,
    hop_two,
    w1_self,
    w1_neigh,
    b1,
    w2_self,
    w2_neigh,
    b2,
):
    height, nodes = features.shape
    seeds = seed_rows.shape[0]
    hid_dev = b1.shape[0]
    hid, depth = w1_self.shape
    cap = want_rows.shape[2]
    fan1 = hop_one.shape[0]
    fan2 = hop_two.shape[0]
    columns = (fan1 + 1) * (seeds // nf)
    vmem = pl.BlockSpec(memory_space=pltpu.VMEM)
    dma = pltpu.SemaphoreType.DMA
    return pl.pallas_call(
        functools.partial(kernel, nd, nf),
        out_shape=pltpu.VMEM((hid_dev, seeds), F32),
        in_specs=[
            pl.BlockSpec(memory_space=pl.ANY),
            vmem,
            vmem,
            pl.BlockSpec(memory_space=pltpu.SMEM),
        ]
        + [pl.BlockSpec(memory_space=pl.ANY)] * 6
        + [vmem] * 2,
        out_specs=vmem,
        scratch_shapes=[
            pltpu.VMEM((height, nodes), BF16),
            pltpu.VMEM(hop_one.shape, jnp.int32),
            pltpu.VMEM(hop_two.shape, jnp.int32),
            pltpu.VMEM(w1_self.shape, BF16),
            pltpu.VMEM(w1_neigh.shape, BF16),
            pltpu.VMEM((nd, nd, cap), jnp.int32),
            pltpu.VMEM((nd, height, cap), BF16),
            pltpu.VMEM((nd, height, cap), BF16),
            pltpu.VMEM((nf, nd, height, cap), BF16),
            pltpu.VMEM((seeds // LANES, height, LANES), BF16),
            pltpu.VMEM((nf, height, LANES), BF16),
            pltpu.VMEM((2, nf, hid_dev, w2_self.shape[0]), BF16),
            pltpu.VMEM((nf, 1, hid_dev), F32),
            pltpu.VMEM((nf, 1, hid_dev), F32),
            pltpu.VMEM((columns // LANES, 16, LANES), jnp.int32),
            pltpu.VMEM((nd * cap, columns), BF16),
            pltpu.VMEM((nd * cap, columns), BF16),
            pltpu.VMEM((depth, nd * cap), BF16),
            pltpu.VMEM((depth, columns), F32),
            pltpu.VMEM((depth, columns), F32),
            pltpu.VMEM((depth, columns), BF16),
            pltpu.VMEM((depth, columns), BF16),
            pltpu.VMEM((hid, 2 * hid), BF16),
            pltpu.VMEM((nf, hid_dev * (seeds // nf) // LANES, LANES), F32),
            pltpu.VMEM((nf, hid_dev * (seeds // nf) // LANES, LANES), F32),
            dma((7,)),
        ]
        + [dma((nd,))] * 4
        + [dma((nd, nf))] * 2
        + [dma((nf,))] * 2
        + [dma((nf, 4))] * 2
        + [dma((nf,))] * 2,
        compiler_params=pltpu.CompilerParams(collective_id=0, has_side_effects=True),
    )(
        features,
        seed_rows.reshape(1, seeds),
        want_rows,
        live_counts,
        hop_one,
        hop_two,
        w1_self,
        w1_neigh,
        w2_self.T,
        w2_neigh.T,
        b1.reshape(1, hid_dev),
        b2.reshape(1, hid_dev),
    )


def solution(mesh):
    return jax.shard_map(
        functools.partial(per_device, mesh.shape["dom"], mesh.shape["feat"]),
        mesh=mesh,
        in_specs=(
            P("feat", "dom"),
            P("dom"),
            P("dom", None, None),
            P("dom", None),
            P(None, "dom"),
            P(None, None, "dom"),
            P(),
            P(),
            P("feat"),
            P(None, "feat"),
            P(None, "feat"),
            P("feat"),
        ),
        out_specs=P("feat", "dom"),
        check_vma=False,
    )
```
